128 devices in a mesh: row: 16 (over x_hi, z, core), col: 8 (over x_lo, y).
Axes of the slice: x: 4 (x_hi: 2, x_lo: 2; x = x_hi * 2 + x_lo), y: 4, z: 4, core: 2. Of those that a mesh axis runs over, the one named last changes fastest.
Arguments:
- tokens: bfloat16 [65536, 6144], P(('row', 'col')), may hold values from -6 to 6
- grad_out: bfloat16 [65536, 6144], P(('row', 'col')), may hold values from -6 to 6
- w_up: bfloat16 [6144, 512], replicated, may hold values from -0.078125 to 0.078125
- w_down: bfloat16 [512, 6144], replicated, may hold values from -0.0390625 to 0.0390625
Outputs:
- up_grad: float32 [6144, 512], P('row', 'col')
- down_grad: float32 [6144, 512], P('row', 'col')
The draws below stay inside these ranges and needn't reach their ends.
All inputs are finite; a program needn't handle non-finite values.
Results may differ from the reference program's by a relative error of at most 0.0041.
Values may be sent and summed in bfloat16 or wider, within the bound.
No kernel may reach another device: no remote copies, remote signals or barrier semaphores. Data moves between devices by JAX's collectives and lax.ppermute only.
A program may use at most 128 MiB of HBM per device.

```python
import math
import jax
import jax.numpy as jnp
from jax import lax

D = 6144
FF = 24576
C = 512
TOK_DEV = 512
TOKENS = 65536
N_ROW = 16
N_COL = 8


def shard_levels(own_key, shape, cuts, least, top_value):
    factor_of, own = 1.0, jax.random.fold_in(own_key, 6)
    for dim, blocks in cuts:
        steps = jnp.exp(jax.random.uniform(jax.random.fold_in(own, dim), (blocks,), jnp.float32, least / len(cuts), top_value / len(cuts)))
        factor_of = factor_of * jnp.repeat(steps, shape[dim] // blocks).reshape([-1 if axis == dim else 1 for axis in range(len(shape))])
    return factor_of


def normal_values(stream_key, dims, spread, most, cuts=(), kind=jnp.bfloat16):
    drawn = jax.random.normal(stream_key, dims, jnp.float32) * spread
    if len(cuts) > 0:
        drawn = shard_levels(stream_key, dims, cuts, -0.22, 0.18) * drawn
    return jnp.clip(drawn, min=-most, max=most).astype(kind)


def setup_inputs(seed: int = 0) -> dict:
    streams_of = jax.random.split(jax.random.key(seed), 5)
    tokens = normal_values(streams_of[0], (TOKENS, D), 1.0, 6.0, ((0, 128),))
    grad_out = normal_values(streams_of[1], (TOKENS, D), 1.0, 6.0, ((0, 128),))
    w_up = normal_values(streams_of[2], (D, C), D ** -0.5, 0.078125)
    w_down = normal_values(streams_of[3], (C, D), FF ** -0.5, 0.0390625)
    return {"tokens": tokens, "grad_out": grad_out, "w_up": w_up, "w_down": w_down}


def gelu_parts(preact):
    cumul = 0.5 * (1.0 + jax.scipy.special.erf(preact / math.sqrt(2.0)))
    density = jnp.exp(-0.5 * preact * preact) / math.sqrt(2.0 * math.pi)
    return (preact * cumul, cumul + preact * density)

def rounded(term):
    levels = term.astype(jnp.bfloat16)
    levels = lax.optimization_barrier(levels)
    return levels.astype(jnp.float32)

def reference(tokens, grad_out, w_up, w_down):

    def one_device(totals, index):
        start = (index * TOK_DEV).astype(jnp.int32)
        own_tok = lax.dynamic_slice_in_dim(tokens, start, TOK_DEV, 0)
        own_grad = lax.dynamic_slice_in_dim(grad_out, start, TOK_DEV, 0)
        preact = jnp.dot(own_tok, w_up, preferred_element_type=jnp.float32)
        act_grad = jnp.dot(own_grad, w_down.T, preferred_element_type=jnp.float32)
        value, slope = gelu_parts(preact)
        act = value.astype(jnp.bfloat16)
        hidden_grad = (act_grad * slope).astype(jnp.bfloat16)
        term_up = jnp.dot(own_tok.T, hidden_grad, preferred_element_type=jnp.float32)
        term_down = jnp.dot(own_grad.T, act, preferred_element_type=jnp.float32)
        return ((totals[0] + rounded(term_up), totals[1] + rounded(term_down)), None)
    zeros = jnp.zeros((D, C), jnp.float32)
    count = N_ROW * N_COL
    (sum_up, sum_down), _ = lax.scan(one_device, (zeros, zeros), jnp.arange(count, dtype=jnp.int32))
    factor = 1.0 / math.sqrt(TOKENS)
    return (sum_up * factor, sum_down * factor)
```

```python
import functools
import math

import jax
import jax.numpy as jnp
from jax import lax
from jax.experimental import pallas as pl
from jax.experimental.pallas import tpu as pltpu
from jax.sharding import PartitionSpec as P

AXES = ("row", "col")
TOK = 512
HID = 512
WIDTH = 6144
LANES = 128
SUB = 64
COLORS = 3
HALF = WIDTH // 2
BF16 = jnp.bfloat16
F32 = jnp.float32


def coords(index):
    row, col = divmod(index, 8)
    xh, rest = divmod(row, 8)
    z, core = divmod(rest, 2)
    xl, y = divmod(col, 4)
    return xh * 2 + xl, y, z, core


def linear(x, y, z, core):
    x, y, z = x % 4, y % 4, z % 4
    return ((x // 2) * 8 + z * 2 + core) * 8 + (x % 2) * 4 + y


def shift(value, axis0, axis1, step):
    pairs = []
    for index in range(128):
        x, y, z, core = coords(index)
        place = {"x": x, "y": y, "z": z}
        place[axis0 if core == 0 else axis1] += step
        pairs.append((index, linear(place["x"], place["y"], place["z"], core)))
    return lax.ppermute(value, AXES, pairs)


def swap(value):
    pairs = []
    for index in range(128):
        x, y, z, core = coords(index)
        pairs.append((index, linear(x, y, z, 1 - core)))
    return lax.ppermute(value, AXES, pairs)


def params(mib, dims=1):
    return pltpu.CompilerParams(
        vmem_limit_bytes=mib * 1024 * 1024, dimension_semantics=("arbitrary",) * dims
    )


def cost(flops, bytes_accessed):
    return pl.CostEstimate(flops=flops, bytes_accessed=bytes_accessed, transcendentals=0)


def pack_partner(meta, step, block_ref, pack_ref):
    core, own_z = meta[0], meta[3]
    xh, z = step // 4, step % 4
    j = (z - own_z + 4) % 4
    for cp in range(2):
        source = pl.multiple_of(cp * 384 + (1 - core) * LANES, LANES)
        target = pl.multiple_of((j * 4 + xh * 2 + cp) * LANES, LANES)
        pack_ref[:, pl.ds(target, LANES)] = block_ref[:, pl.ds(source, LANES)]
    source = pl.multiple_of((1 - core) * 384 + 2 * LANES, LANES)
    target = pl.multiple_of((16 + j * 2 + xh) * LANES, LANES)
    pack_ref[:, pl.ds(target, LANES)] = block_ref[:, pl.ds(source, LANES)]


def act_grad_kernel(meta, grad_ref, w_ref, out_ref, pack_ref):
    step = pl.program_id(0)
    part = lax.dot_general(
        grad_ref[...], w_ref[...], (((1,), (1,)), ((), ())), preferred_element_type=F32
    )

    @pl.when(step == 0)
    def _():
        out_ref[...] = part

    @pl.when(step > 0)
    def _():
        out_ref[...] += part

    pack_partner(meta, step, grad_ref, pack_ref)


def hidden_kernel(meta, tok_ref, w_ref, act_grad_ref, hid_ref, pack_ref, acc_ref):
    step = pl.program_id(0)
    part = jnp.dot(tok_ref[...], w_ref[...], preferred_element_type=F32)

    @pl.when(step == 0)
    def _():
        acc_ref[...] = part

    @pl.when(step > 0)
    def _():
        acc_ref[...] += part

    pack_partner(meta, step, tok_ref, pack_ref)

    @pl.when(step == pl.num_programs(0) - 1)
    def _():
        preact = acc_ref[...]
        cumul = 0.5 * (1.0 + lax.erf(preact * (1.0 / math.sqrt(2.0))))
        density = jnp.exp(-0.5 * preact * preact) * (1.0 / math.sqrt(2.0 * math.pi))
        act = preact * cumul
        hidden = act_grad_ref[...] * (cumul + preact * density)
        hid_ref[:, 0:TOK] = act.T.astype(BF16)
        hid_ref[:, TOK : 2 * TOK] = hidden.T.astype(BF16)


def term_kernel(meta, *refs, aliased):
    lhs_own, lhs_peer, b0, b1, b2, b3, peer = refs[:7]
    refs = refs[7 + (8 if aliased else 0) :]
    major, minor, scr = refs[:4], refs[4:8], refs[8]
    step = pl.program_id(0)
    core, own_x, own_y = meta[0], meta[1], meta[2]
    own = jnp.concatenate([b0[...], b1[...], b2[...], b3[...]], axis=1)
    acc = jnp.dot(lhs_own[...], own, preferred_element_type=F32)
    acc += jnp.dot(lhs_peer[...], peer[...], preferred_element_type=F32)
    acc = acc.astype(BF16)
    for q in range(4):
        scr[q] = acc[:, q * LANES : (q + 1) * LANES]

    def rows(x, y):
        return pl.ds(pl.multiple_of((x % 2) * 256 + y * SUB, SUB), SUB)

    @pl.when(step < 4)
    def _():
        for d in range(4):
            for w in range(4):
                x = (own_x + jnp.where(core == 0, d, w)) % 4
                y = (own_y + jnp.where(core == 0, w, d)) % 4
                for cp in range(2):
                    major[d][0, 0, cp, w] = scr[(x // 2) * 2 + cp, rows(x, y), :]

    for half in range(2):

        @pl.when(step == 4 + half)
        def _():
            for jj in range(2):
                for xo in range(4):
                    x = (own_x + xo) % 4
                    for yo in range(4):
                        y = (own_y + yo) % 4
                        minor[half * 2 + jj][0, xo, yo] = scr[jj * 2 + x // 2, rows(x, y), :]


def term_call(meta, which, hid, hid_peer, full, pack_peer, buffers):
    def own_spec(q):
        def index(s, m):
            core, own_z = m[0], m[3]
            z_major = (own_z + s) % 4
            r_major = (q // 2) * 8 + z_major * 2 + q % 2
            z_minor = (own_z + (s - 4) * 2 + q // 2 + 4) % 4
            r_minor = (q % 2) * 8 + z_minor * 2 + core
            return 0, jnp.where(s < 4, r_major * COLORS + core, r_minor * COLORS + 2)

        return pl.BlockSpec((TOK, LANES), index)

    lhs = pl.BlockSpec((HID, TOK), lambda s, m: (0, which))
    in_specs = [lhs, lhs] + [own_spec(q) for q in range(4)]
    in_specs.append(pl.BlockSpec((TOK, 4 * LANES), lambda s, m: (0, s)))
    operands = [meta, hid, hid_peer, full, full, full, full, pack_peer]
    aliases = {}
    if buffers is not None:
        in_specs += [pl.BlockSpec(memory_space=pl.ANY)] * 8
        aliases = {len(operands) + i: i for i in range(8)}
        operands += list(buffers)
    major_spec = pl.BlockSpec(
        (1, 1, 2, 4, SUB, LANES), lambda s, m: (which, jnp.minimum(s, 3), 0, 0, 0, 0)
    )
    minor_spec = pl.BlockSpec((1, 4, 4, SUB, LANES), lambda s, m: (which, 0, 0, 0, 0))
    return pl.pallas_call(
        functools.partial(term_kernel, aliased=buffers is not None),
        grid_spec=pltpu.PrefetchScalarGridSpec(
            num_scalar_prefetch=1,
            grid=(6,),
            in_specs=in_specs,
            out_specs=[major_spec] * 4 + [minor_spec] * 4,
            scratch_shapes=[pltpu.VMEM((4, HID, LANES), BF16)],
        ),
        out_shape=[jax.ShapeDtypeStruct((2, 4, 2, 4, SUB, LANES), BF16)] * 4
        + [jax.ShapeDtypeStruct((2, 4, 4, SUB, LANES), BF16)] * 4,
        input_output_aliases=aliases,
        compiler_params=params(24),
        cost_estimate=cost(4 * TOK * HID * HALF, 12 * 1024 * 1024),
        name=("down_term", "up_term")[which],
    )(*operands)


def total(parts, index):
    out = parts[0][index].astype(F32)
    for part in parts[1:]:
        out += part[index].astype(F32)
    return out


def sum1_kernel(meta, *refs):
    major, minor = refs[0:4], refs[4:8]
    out_major, out_minor = refs[8:12], refs[12:16]
    core = meta[0]
    for e in range(4):

        def body(f, _):
            j = jnp.where(core == 0, f, e)
            w = jnp.where(core == 0, e, f)
            for t in range(2):
                for cp in range(2):
                    out_major[e][t, f, cp] = total(major, (t, j, cp, w)).astype(BF16)
                out_minor[e][t, f] = total(minor, (t, e, f)).astype(BF16)
            return 0

        lax.fori_loop(0, 4, body, 0)


def sum2_kernel(meta, *refs):
    major, minor = refs[0:4], refs[4:8]
    out_major, out_minor = refs[8:12], refs[12:16]
    for f in range(4):
        for t in range(2):
            for cp in range(2):
                out_major[f][t, cp] = total(major, (t, f, cp)).astype(BF16)
            out_minor[f][t] = total(minor, (t, f)).astype(BF16)


def sum3_kernel(meta, *refs):
    major, minor = refs[0:4], refs[4:8]
    keep, send, rest = refs[8:11]
    core = meta[0]
    for t in range(2):
        keep[t] = total(major, (t, core))
        send[t] = total(major, (t, 1 - core))
        rest[t] = total(minor, (t,))


def final_kernel(meta, keep, got, rest, up_ref, down_ref, *, factor):
    first = meta[0] == 0
    for t, out in ((0, down_ref), (1, up_ref)):
        out[:, 0:LANES] = jnp.where(first, keep[t], got[t]) * factor
        out[:, LANES : 2 * LANES] = jnp.where(first, got[t], keep[t]) * factor
        out[:, 2 * LANES : 3 * LANES] = rest[t] * factor


def whole_call(kernel, meta, operands, shapes, mib, name):
    vmem = pl.BlockSpec(memory_space=pltpu.VMEM)
    return pl.pallas_call(
        kernel,
        in_specs=[pl.BlockSpec(memory_space=pltpu.SMEM)] + [vmem] * len(operands),
        out_specs=[vmem] * len(shapes),
        out_shape=shapes,
        compiler_params=pltpu.CompilerParams(vmem_limit_bytes=mib * 1024 * 1024),
        name=name,
    )(meta, *operands)


def exchange(major, minor, axis0, axis1, axis2):
    got_major, got_minor = [major[0]], [minor[0]]
    for d in (2, 1, 3):
        got_major.append(shift(major[d], axis0, axis1, d))
        got_minor.append(shift(minor[d], axis2, axis2, d))
    return got_major + got_minor


def local(tokens, grad_out, w_up, w_down):
    index = lax.axis_index(AXES)
    place = jnp.arange(4, dtype=jnp.int32)
    xh, z, core = index // 64, (index // 16) % 4, (index // 8) % 2
    xl, y = (index // 4) % 2, index % 4
    meta = jnp.where(place == 0, core, jnp.where(place == 1, xh * 2 + xl, jnp.where(place == 2, y, z)))
    meta = meta.astype(jnp.int32)

    width = 2 * COLORS * LANES
    steps = WIDTH // width
    act_grad, pack_grad = pl.pallas_call(
        act_grad_kernel,
        grid_spec=pltpu.PrefetchScalarGridSpec(
            num_scalar_prefetch=1,
            grid=(steps,),
            in_specs=[
                pl.BlockSpec((TOK, width), lambda s, m: (0, s)),
                pl.BlockSpec((HID, width), lambda s, m: (0, s)),
            ],
            out_specs=[
                pl.BlockSpec((TOK, HID), lambda s, m: (0, 0)),
                pl.BlockSpec((TOK, HALF), lambda s, m: (0, 0)),
            ],
        ),
        out_shape=[
            jax.ShapeDtypeStruct((TOK, HID), F32),
            jax.ShapeDtypeStruct((TOK, HALF), BF16),
        ],
        compiler_params=params(24),
        cost_estimate=cost(2 * TOK * HID * WIDTH, 16 * 1024 * 1024),
        name="act_grad",
    )(meta, grad_out, w_down)
    peer_grad = swap(pack_grad)

    hid, pack_tok = pl.pallas_call(
        hidden_kernel,
        grid_spec=pltpu.PrefetchScalarGridSpec(
            num_scalar_prefetch=1,
            grid=(steps,),
            in_specs=[
                pl.BlockSpec((TOK, width), lambda s, m: (0, s)),
                pl.BlockSpec((width, HID), lambda s, m: (s, 0)),
                pl.BlockSpec((TOK, HID), lambda s, m: (0, 0)),
            ],
            out_specs=[
                pl.BlockSpec((HID, 2 * TOK), lambda s, m: (0, 0)),
                pl.BlockSpec((TOK, HALF), lambda s, m: (0, 0)),
            ],
            scratch_shapes=[pltpu.VMEM((TOK, HID), F32)],
        ),
        out_shape=[
            jax.ShapeDtypeStruct((HID, 2 * TOK), BF16),
            jax.ShapeDtypeStruct((TOK, HALF), BF16),
        ],
        compiler_params=params(28),
        cost_estimate=cost(2 * TOK * HID * WIDTH, 18 * 1024 * 1024),
        name="hidden",
    )(meta, tokens, w_up, act_grad)
    hid_peer = swap(hid)
    peer_tok = swap(pack_tok)

    buffers = term_call(meta, 0, hid, hid_peer, grad_out, peer_grad, None)
    buffers = term_call(meta, 1, hid, hid_peer, tokens, peer_tok, buffers)

    got = exchange(buffers[:4], buffers[4:], "x", "y", "z")
    out = whole_call(
        sum1_kernel, meta, got,
        [jax.ShapeDtypeStruct((2, 4, 2, SUB, LANES), BF16)] * 4
        + [jax.ShapeDtypeStruct((2, 4, SUB, LANES), BF16)] * 4,
        24, "sum1",
    )
    got = exchange(out[:4], out[4:], "y", "z", "x")
    out = whole_call(
        sum2_kernel, meta, got,
        [jax.ShapeDtypeStruct((2, 2, SUB, LANES), BF16)] * 4
        + [jax.ShapeDtypeStruct((2, SUB, LANES), BF16)] * 4,
        16, "sum2",
    )
    got = exchange(out[:4], out[4:], "z", "x", "y")
    keep, send, rest = whole_call(
        sum3_kernel, meta, got, [jax.ShapeDtypeStruct((2, SUB, LANES), F32)] * 3, 16, "sum3"
    )
    total_tokens = tokens.shape[0] * lax.axis_size("row") * lax.axis_size("col")
    up, down = whole_call(
        functools.partial(final_kernel, factor=1.0 / math.sqrt(total_tokens)),
        meta, [keep, swap(send), rest],
        [jax.ShapeDtypeStruct((SUB, COLORS * LANES), F32)] * 2, 16, "final",
    )
    return up.T, down.T


def solution(mesh):
    placed = (P(AXES, None), P(AXES, None), P(), P())
    return jax.shard_map(
        local,
        mesh=mesh,
        in_specs=placed,
        out_specs=(P("row", "col"), P("row", "col")),
        check_vma=False,
    )
```

```python
import functools
import math

import jax
import jax.numpy as jnp
from jax import lax
from jax.experimental import pallas as pl
from jax.experimental.pallas import tpu as pltpu
from jax.sharding import PartitionSpec as P


AXES = ("row", "col")
TOK = 512
HID = 512
WIDTH = 6144
LANES = 128
SUB = 64
COLORS = 3
HALF = WIDTH // 2
BF16 = jnp.bfloat16
F32 = jnp.float32


def coords(index):
    row, col = divmod(index, 8)
    xh, rest = divmod(row, 8)
    z, core = divmod(rest, 2)
    xl, y = divmod(col, 4)
    return xh * 2 + xl, y, z, core


def linear(x, y, z, core):
    x, y, z = x % 4, y % 4, z % 4
    return ((x // 2) * 8 + z * 2 + core) * 8 + (x % 2) * 4 + y


def shift(value, axis0, axis1, step):
    pairs = []
    for index in range(128):
        x, y, z, core = coords(index)
        place = {"x": x, "y": y, "z": z}
        place[axis0 if core == 0 else axis1] += step
        pairs.append((index, linear(place["x"], place["y"], place["z"], core)))
    return lax.ppermute(value, AXES, pairs)


def swap(value):
    pairs = []
    for index in range(128):
        x, y, z, core = coords(index)
        pairs.append((index, linear(x, y, z, 1 - core)))
    return lax.ppermute(value, AXES, pairs)


def limit(mib):
    return pltpu.CompilerParams(vmem_limit_bytes=mib * 1024 * 1024)


def cost(flops, bytes_accessed):
    return pl.CostEstimate(flops=flops, bytes_accessed=bytes_accessed, transcendentals=0)


VMEM = pl.BlockSpec(memory_space=pltpu.VMEM)
SMEM = pl.BlockSpec(memory_space=pltpu.SMEM)
ANY = pl.BlockSpec(memory_space=pl.ANY)
LIM = 12
CHUNK = 2 * COLORS * LANES
CHUNKS = WIDTH // CHUNK


def pack_columns(meta, step, block_ref, peer_ref):
    core, own_z = meta[0], meta[3]
    xh, z = step // 4, step % 4
    j = (z - own_z + 4) % 4
    base = step * CHUNK
    for cp in range(2):
        source = pl.multiple_of(base + cp * 384 + (1 - core) * LANES, LANES)
        target = pl.multiple_of((j * 4 + xh * 2 + cp) * LANES, LANES)
        peer_ref[:, pl.ds(target, LANES)] = block_ref[:, pl.ds(source, LANES)]
    source = pl.multiple_of(base + (1 - core) * 384 + 2 * LANES, LANES)
    target = pl.multiple_of((16 + j * 2 + xh) * LANES, LANES)
    peer_ref[:, pl.ds(target, LANES)] = block_ref[:, pl.ds(source, LANES)]


def preact_kernel(meta, tok_ref, w_ref, out_ref, peer_ref):
    out_ref[...] = jnp.zeros_like(out_ref)

    def body(pair, _):
        at = pl.ds(pl.multiple_of(pair * 2 * CHUNK, 2 * CHUNK), 2 * CHUNK)
        out_ref[...] += jnp.dot(tok_ref[:, at], w_ref[at, :], preferred_element_type=F32)
        for half in range(2):
            pack_columns(meta, pair * 2 + half, tok_ref, peer_ref)
        return 0

    lax.fori_loop(0, CHUNKS // 2, body, 0)


def hidden_kernel(meta, grad_ref, w_ref, preact_ref, hid_ref, peer_ref, acc_ref, slope_ref):
    acc_ref[...] = jnp.zeros_like(acc_ref)

    def body(pair, _):
        rows = pl.ds(pl.multiple_of(pair * LANES, LANES), LANES)
        preact = preact_ref[rows, :].T
        cumul = 0.5 * (1.0 + lax.erf(preact * (1.0 / math.sqrt(2.0))))
        density = jnp.exp(-0.5 * preact * preact) * (1.0 / math.sqrt(2.0 * math.pi))
        hid_ref[:, rows] = (preact * cumul).astype(BF16)
        slope_ref[:, rows] = cumul + preact * density
        at = pl.ds(pl.multiple_of(pair * 2 * CHUNK, 2 * CHUNK), 2 * CHUNK)
        acc_ref[...] += lax.dot_general(
            w_ref[:, at], grad_ref[:, at], (((1,), (1,)), ((), ())), preferred_element_type=F32
        )
        for half in range(2):
            pack_columns(meta, pair * 2 + half, grad_ref, peer_ref)
        return 0

    lax.fori_loop(0, CHUNKS // 2, body, 0)
    hid_ref[:, TOK : 2 * TOK] = (acc_ref[...] * slope_ref[...]).astype(BF16)


def term_kernel(meta, *refs, which, first):
    hid, hid_peer, full, peer = refs[:4]
    refs = refs[4 + (0 if first else 6) :]
    out_at = {0: (0, which), 1: (1, which), 3: (2, which), 2: (6, 0)}
    major = {d: refs[i].at[t] for d, (i, t) in out_at.items()}
    minor = {d: refs[i + (3 if d != 2 else 1)].at[t] for d, (i, t) in out_at.items()}
    scr = refs[8]
    core, own_x, own_y, own_z = meta[0], meta[1], meta[2], meta[3]
    lhs = slice((which == 1) * TOK, (which == 1) * TOK + TOK)

    def rows(x, y):
        return pl.ds(pl.multiple_of((x % 2) * 256 + y * SUB, SUB), SUB)

    def matmul(step, slot):
        tiles = []
        for q in range(4):
            if step < 4:
                group = (q // 2) * 8 + (own_z + step) % 4 * 2 + q % 2
                column = group * 384 + core * LANES
            else:
                group = (q % 2) * 8 + (own_z + (step - 4) * 2 + q // 2) % 4 * 2 + core
                column = group * 384 + 2 * LANES
            tiles.append(full[:, pl.ds(pl.multiple_of(column, LANES), LANES)])
        own = jnp.concatenate(tiles, axis=1)
        acc = jnp.dot(hid[:, lhs], own, preferred_element_type=F32)
        other = peer[:, step * 4 * LANES : (step + 1) * 4 * LANES]
        acc += jnp.dot(hid_peer[:, lhs], other, preferred_element_type=F32)
        acc = acc.astype(BF16)
        for q in range(4):
            scr[slot, q] = acc[:, q * LANES : (q + 1) * LANES]

    def scatter(step, slot):
        if step < 4:
            for d in range(4):
                for w in range(4):
                    x = (own_x + jnp.where(core == 0, d, w)) % 4
                    y = (own_y + jnp.where(core == 0, w, d)) % 4
                    for cp in range(2):
                        major[d][step, cp, w] = scr[slot, (x // 2) * 2 + cp, rows(x, y), :]
            return
        for jj in range(2):
            for xo in range(4):
                x = (own_x + xo) % 4
                for yo in range(4):
                    y = (own_y + yo) % 4
                    minor[(step - 4) * 2 + jj][xo, yo] = scr[slot, jj * 2 + x // 2, rows(x, y), :]

    matmul(0, 0)
    for step in range(1, 6):
        matmul(step, step % 2)
        scatter(step - 1, (step - 1) % 2)
    scatter(5, 1)


MAJOR1 = (4, 2, 4, SUB, LANES)
MINOR1 = (4, 4, SUB, LANES)


def bf16(*dims):
    return jax.ShapeDtypeStruct(dims, BF16)


def term_call(meta, which, hid, hid_peer, full, peer, buffers):
    operands = [meta, hid, hid_peer, full, peer]
    aliases = {}
    if buffers is not None:
        aliases = {len(operands) + i: i for i in range(6)}
        operands += list(buffers)
    return pl.pallas_call(
        functools.partial(term_kernel, which=which, first=buffers is None),
        in_specs=[SMEM] + [VMEM] * (len(operands) - 1),
        out_specs=[VMEM] * 8,
        out_shape=[bf16(2, *MAJOR1)] * 3 + [bf16(2, *MINOR1)] * 3 + [bf16(1, *MAJOR1), bf16(1, *MINOR1)],
        scratch_shapes=[pltpu.VMEM((2, 4, HID, LANES), BF16)],
        input_output_aliases=aliases,
        compiler_params=limit(LIM),
        cost_estimate=cost(4 * TOK * HID * HALF, 12 * 1024 * 1024),
    )(*operands)


def total(pieces):
    out = pieces[0].astype(F32)
    for piece in pieces[1:]:
        out += piece.astype(F32)
    return out


def major1_kernel(meta, *refs):
    core = meta[0]
    parts, two, out = refs[:3], refs[3:5], refs[5:9]
    for e in range(4):

        def body(f, _):
            j = jnp.where(core == 0, f, e)
            w = jnp.where(core == 0, e, f)
            for t in range(2):
                for cp in range(2):
                    pieces = [part[t, j, cp, w] for part in parts] + [two[t][0, j, cp, w]]
                    out[e][t, f, cp] = total(pieces).astype(BF16)
            return 0

        lax.fori_loop(0, 4, body, 0)


def minor1_kernel(meta, *refs):
    parts, two, out = refs[:3], refs[3:5], refs[6:10]
    for e in range(4):

        def body(f, _):
            for t in range(2):
                pieces = [part[t, e, f] for part in parts] + [two[t][0, e, f]]
                out[e][t, f] = total(pieces).astype(BF16)
            return 0

        lax.fori_loop(0, 4, body, 0)


def major2_kernel(meta, *refs):
    parts, out = refs[:4], refs[5:9]
    for f in range(4):
        for t in range(2):
            for cp in range(2):
                out[f][t, cp] = total([part[t, f, cp] for part in parts]).astype(BF16)


def minor2_kernel(meta, *refs):
    parts, out = refs[:4], refs[5:9]
    for f in range(4):
        for t in range(2):
            out[f][t] = total([part[t, f] for part in parts]).astype(BF16)


def major3_kernel(meta, *refs):
    parts, (keep, send) = refs[:4], refs[5:7]
    core = meta[0]
    for t in range(2):
        keep[t] = total([part[t, core] for part in parts])
        send[t] = total([part[t, 1 - core] for part in parts])


def final_kernel(meta, keep, got, p0, p1, p2, p3, up_ref, down_ref, *, factor):
    first = meta[0] == 0
    for t, out in ((0, down_ref), (1, up_ref)):
        out[:, 0:LANES] = jnp.where(first, keep[t], got[t]) * factor
        out[:, LANES : 2 * LANES] = jnp.where(first, got[t], keep[t]) * factor
        out[:, 2 * LANES : 3 * LANES] = total([part[t] for part in (p0, p1, p2, p3)]) * factor


def sum_call(kernel, meta, operands, shapes, after=None):
    in_specs = [SMEM] + [VMEM] * len(operands)
    operands = [meta, *operands]
    if after is not None:
        in_specs.append(ANY)
        operands.append(after)
    return pl.pallas_call(
        kernel,
        in_specs=in_specs,
        out_specs=[VMEM] * len(shapes),
        out_shape=shapes,
        compiler_params=limit(LIM),
    )(*operands)


def ring(parts, axis0, axis1):
    return [parts[0]] + [shift(parts[d], axis0, axis1, d) for d in (2, 1, 3)]


def local(tokens, grad_out, w_up, w_down):
    index = lax.axis_index(AXES)
    place = jnp.arange(4, dtype=jnp.int32)
    xh, z, core = index // 64, (index // 16) % 4, (index // 8) % 2
    xl, y = (index // 4) % 2, index % 4
    meta = jnp.where(place == 0, core, jnp.where(place == 1, xh * 2 + xl, jnp.where(place == 2, y, z)))
    meta = meta.astype(jnp.int32)

    preact, pack_tok = pl.pallas_call(
        preact_kernel,
        in_specs=[SMEM, VMEM, VMEM],
        out_specs=[VMEM] * 2,
        out_shape=[jax.ShapeDtypeStruct((TOK, HID), F32), bf16(TOK, HALF)],
        compiler_params=limit(LIM),
        cost_estimate=cost(2 * TOK * HID * WIDTH, 16 * 1024 * 1024),
        name="preact",
    )(meta, tokens, w_up)
    peer_tok = swap(pack_tok)

    hid, pack_grad = pl.pallas_call(
        hidden_kernel,
        in_specs=[SMEM, VMEM, VMEM, VMEM],
        out_specs=[VMEM] * 2,
        out_shape=[bf16(HID, 2 * TOK), bf16(TOK, HALF)],
        scratch_shapes=[pltpu.VMEM((HID, TOK), F32), pltpu.VMEM((HID, TOK), F32)],
        compiler_params=limit(LIM),
        cost_estimate=cost(2 * TOK * HID * WIDTH, 18 * 1024 * 1024),
        name="hidden",
    )(meta, grad_out, w_down, preact)
    hid_peer = swap(hid)
    peer_grad = swap(pack_grad)

    out = term_call(meta, 1, hid, hid_peer, tokens, peer_tok, None)
    major_up = shift(out[6], "x", "y", 2)
    minor_up = shift(out[7], "z", "z", 2)
    out = term_call(meta, 0, hid, hid_peer, grad_out, peer_grad, out[:6])

    major_two = [shift(out[6], "x", "y", 2), major_up]
    minor_two = [shift(out[7], "z", "z", 2), minor_up]
    major = [out[0], shift(out[1], "x", "y", 1), shift(out[2], "x", "y", 3)]
    minor = [out[3], shift(out[4], "z", "z", 1), shift(out[5], "z", "z", 3)]
    major = sum_call(major1_kernel, meta, major + major_two, [bf16(2, 4, 2, SUB, LANES)] * 4)
    minor = sum_call(minor1_kernel, meta, minor + minor_two, [bf16(2, 4, SUB, LANES)] * 4, major[0])
    major = ring(major, "y", "z")
    last = minor[0]
    minor = ring(minor, "x", "x")
    major = sum_call(major2_kernel, meta, major, [bf16(2, 2, SUB, LANES)] * 4, last)
    minor = sum_call(minor2_kernel, meta, minor, [bf16(2, SUB, LANES)] * 4, major[0])
    major = ring(major, "z", "x")
    last = minor[0]
    minor = ring(minor, "y", "y")
    keep, send = sum_call(
        major3_kernel, meta, major, [jax.ShapeDtypeStruct((2, SUB, LANES), F32)] * 2, last
    )
    total_tokens = tokens.shape[0] * lax.axis_size("row") * lax.axis_size("col")
    up, down = sum_call(
        functools.partial(final_kernel, factor=1.0 / math.sqrt(total_tokens)),
        meta, [keep, swap(send)] + minor,
        [jax.ShapeDtypeStruct((SUB, COLORS * LANES), F32)] * 2,
    )
    return up.T, down.T


def solution(mesh):
    placed = (P(AXES, None), P(AXES, None), P(), P())
    return jax.shard_map(
        local,
        mesh=mesh,
        in_specs=placed,
        out_specs=(P("row", "col"), P("row", "col")),
        check_vma=False,
    )
```

```python
import functools
import math

import jax
import jax.numpy as jnp
from jax import lax
from jax.experimental import pallas as pl
from jax.experimental.pallas import tpu as pltpu
from jax.sharding import PartitionSpec as P


AXES = ("row", "col")
TOK = 512
HID = 512
WIDTH = 6144
LANES = 128
SUB = 64
COLORS = 3
HALF = WIDTH // 2
BF16 = jnp.bfloat16
F32 = jnp.float32


def coords(index):
    row, col = divmod(index, 8)
    xh, rest = divmod(row, 8)
    z, core = divmod(rest, 2)
    xl, y = divmod(col, 4)
    return xh * 2 + xl, y, z, core


def linear(x, y, z, core):
    x, y, z = x % 4, y % 4, z % 4
    return ((x // 2) * 8 + z * 2 + core) * 8 + (x % 2) * 4 + y


def shift(value, axis0, axis1, step):
    pairs = []
    for index in range(128):
        x, y, z, core = coords(index)
        place = {"x": x, "y": y, "z": z}
        place[axis0 if core == 0 else axis1] += step
        pairs.append((index, linear(place["x"], place["y"], place["z"], core)))
    return lax.ppermute(value, AXES, pairs)


def swap(value):
    pairs = []
    for index in range(128):
        x, y, z, core = coords(index)
        pairs.append((index, linear(x, y, z, 1 - core)))
    return lax.ppermute(value, AXES, pairs)


def limit(mib):
    return pltpu.CompilerParams(vmem_limit_bytes=mib * 1024 * 1024)


def cost(flops, bytes_accessed):
    return pl.CostEstimate(flops=flops, bytes_accessed=bytes_accessed, transcendentals=0)


VMEM = pl.BlockSpec(memory_space=pltpu.VMEM)
SMEM = pl.BlockSpec(memory_space=pltpu.SMEM)
ANY = pl.BlockSpec(memory_space=pl.ANY)
LIM = 12
CHUNK = 2 * COLORS * LANES
SPAN = 2 * CHUNK
SPANS = WIDTH // SPAN


def pack_columns(meta, step, block_ref, peer_ref):
    core, own_z = meta[0], meta[3]
    xh, z = step // 4, step % 4
    j = (z - own_z + 4) % 4
    base = step * CHUNK
    for cp in range(2):
        source = pl.multiple_of(base + cp * 384 + (1 - core) * LANES, LANES)
        target = pl.multiple_of((j * 4 + xh * 2 + cp) * LANES, LANES)
        peer_ref[:, pl.ds(target, LANES)] = block_ref[:, pl.ds(source, LANES)]
    source = pl.multiple_of(base + (1 - core) * 384 + 2 * LANES, LANES)
    target = pl.multiple_of((16 + j * 2 + xh) * LANES, LANES)
    peer_ref[:, pl.ds(target, LANES)] = block_ref[:, pl.ds(source, LANES)]


def span(step):
    return pl.ds(pl.multiple_of(step * SPAN, SPAN), SPAN)


def copies(rows_ref, w_ref, w_axis, rows_buf, w_buf, sems):
    def pair(step):
        w_at = (span(step), slice(None)) if w_axis == 0 else (slice(None), span(step))
        return (
            pltpu.make_async_copy(rows_ref.at[:, span(step)], rows_buf.at[:, span(step)], sems.at[0, step]),
            pltpu.make_async_copy(w_ref.at[*w_at], w_buf.at[*w_at], sems.at[1, step]),
        )

    return pair


def preact_kernel(meta, tok_ref, w_ref, out_ref, peer_ref, tok_buf, w_buf, sems):
    pair = copies(tok_ref, w_ref, 0, tok_buf, w_buf, sems)
    for step in range(SPANS):
        for copy in pair(step):
            copy.start()
    out_ref[...] = jnp.zeros_like(out_ref)

    def body(step, _):
        for copy in pair(step):
            copy.wait()
        out_ref[...] += jnp.dot(tok_buf[:, span(step)], w_buf[span(step), :], preferred_element_type=F32)
        for half in range(2):
            pack_columns(meta, step * 2 + half, tok_buf, peer_ref)
        return 0

    lax.fori_loop(0, SPANS, body, 0)


def hidden_kernel(
    meta, grad_ref, w_ref, preact_ref, hid_ref, peer_ref, acc_ref, slope_ref, grad_buf, w_buf, sems
):
    pair = copies(grad_ref, w_ref, 1, grad_buf, w_buf, sems)
    for step in range(SPANS):
        for copy in pair(step):
            copy.start()
    acc_ref[...] = jnp.zeros_like(acc_ref)

    def body(step, _):
        for copy in pair(step):
            copy.wait()
        rows = pl.ds(pl.multiple_of(step * LANES, LANES), LANES)
        preact = preact_ref[rows, :].T
        cumul = 0.5 * (1.0 + lax.erf(preact * (1.0 / math.sqrt(2.0))))
        density = jnp.exp(-0.5 * preact * preact) * (1.0 / math.sqrt(2.0 * math.pi))
        hid_ref[:, rows] = (preact * cumul).astype(BF16)
        slope_ref[:, rows] = cumul + preact * density
        acc_ref[...] += lax.dot_general(
            w_buf[:, span(step)], grad_buf[:, span(step)], (((1,), (1,)), ((), ())), preferred_element_type=F32
        )
        for half in range(2):
            pack_columns(meta, step * 2 + half, grad_buf, peer_ref)
        return 0

    lax.fori_loop(0, SPANS, body, 0)
    hid_ref[:, TOK : 2 * TOK] = (acc_ref[...] * slope_ref[...]).astype(BF16)


def term_kernel(meta, *refs, which):
    hid, hid_peer, full, peer = refs[:4]
    major, minor, scr = refs[4:8], refs[8:12], refs[12]
    core, own_x, own_y, own_z = meta[0], meta[1], meta[2], meta[3]
    lhs = slice((which == 1) * TOK, (which == 1) * TOK + TOK)

    def rows(x, y):
        return pl.ds(pl.multiple_of((x % 2) * 256 + y * SUB, SUB), SUB)

    def matmul(step, slot):
        tiles = []
        for q in range(4):
            if step < 4:
                group = (q // 2) * 8 + (own_z + step) % 4 * 2 + q % 2
                column = group * 384 + core * LANES
            else:
                group = (q % 2) * 8 + (own_z + (step - 4) * 2 + q // 2) % 4 * 2 + core
                column = group * 384 + 2 * LANES
            tiles.append(full[:, pl.ds(pl.multiple_of(column, LANES), LANES)])
        own = jnp.concatenate(tiles, axis=1)
        acc = jnp.dot(hid[:, lhs], own, preferred_element_type=F32)
        other = peer[:, step * 4 * LANES : (step + 1) * 4 * LANES]
        acc += jnp.dot(hid_peer[:, lhs], other, preferred_element_type=F32)
        acc = acc.astype(BF16)
        for q in range(4):
            scr[slot, q] = acc[:, q * LANES : (q + 1) * LANES]

    def scatter(step, slot):
        if step < 4:
            for d in range(4):
                for w in range(4):
                    x = (own_x + jnp.where(core == 0, d, w)) % 4
                    y = (own_y + jnp.where(core == 0, w, d)) % 4
                    for cp in range(2):
                        major[d][step, cp, w] = scr[slot, (x // 2) * 2 + cp, rows(x, y), :]
            return
        for jj in range(2):
            for xo in range(4):
                x = (own_x + xo) % 4
                for yo in range(4):
                    y = (own_y + yo) % 4
                    minor[(step - 4) * 2 + jj][xo, yo] = scr[slot, jj * 2 + x // 2, rows(x, y), :]

    matmul(0, 0)
    for step in range(1, 6):
        matmul(step, step % 2)
        scatter(step - 1, (step - 1) % 2)
    scatter(5, 1)


MAJOR1 = (4, 2, 4, SUB, LANES)
MINOR1 = (4, 4, SUB, LANES)


def bf16(*dims):
    return jax.ShapeDtypeStruct(dims, BF16)


def term_call(meta, which, hid, hid_peer, full, peer):
    return pl.pallas_call(
        functools.partial(term_kernel, which=which),
        in_specs=[SMEM] + [VMEM] * 4,
        out_specs=[VMEM] * 8,
        out_shape=[bf16(*MAJOR1)] * 4 + [bf16(*MINOR1)] * 4,
        scratch_shapes=[pltpu.VMEM((2, 4, HID, LANES), BF16)],
        compiler_params=limit(LIM),
        cost_estimate=cost(4 * TOK * HID * HALF, 12 * 1024 * 1024),
    )(meta, hid, hid_peer, full, peer)


def total(pieces):
    out = pieces[0].astype(F32)
    for piece in pieces[1:]:
        out += piece.astype(F32)
    return out


def major1_kernel(meta, *refs):
    core = meta[0]
    terms, out = (refs[0:4], refs[4:8]), refs[8:12]
    for e in range(4):

        def body(f, _):
            j = jnp.where(core == 0, f, e)
            w = jnp.where(core == 0, e, f)
            for t in range(2):
                for cp in range(2):
                    out[e][t, f, cp] = total([part[j, cp, w] for part in terms[t]]).astype(BF16)
            return 0

        lax.fori_loop(0, 4, body, 0)


def minor1_kernel(meta, *refs):
    terms, out = (refs[0:4], refs[4:8]), refs[9:13]
    for e in range(4):

        def body(f, _):
            for t in range(2):
                out[e][t, f] = total([part[e, f] for part in terms[t]]).astype(BF16)
            return 0

        lax.fori_loop(0, 4, body, 0)


def major2_kernel(meta, *refs):
    parts, out = refs[:4], refs[5:9]
    for f in range(4):
        for t in range(2):
            for cp in range(2):
                out[f][t, cp] = total([part[t, f, cp] for part in parts]).astype(BF16)


def minor2_kernel(meta, *refs):
    parts, out = refs[:4], refs[5:9]
    for f in range(4):
        for t in range(2):
            out[f][t] = total([part[t, f] for part in parts]).astype(BF16)


def major3_kernel(meta, *refs):
    parts, (keep, send) = refs[:4], refs[5:7]
    core = meta[0]
    for t in range(2):
        keep[t] = total([part[t, core] for part in parts])
        send[t] = total([part[t, 1 - core] for part in parts])


def final_kernel(meta, keep, got, p0, p1, p2, p3, up_ref, down_ref, *, factor):
    first = meta[0] == 0
    for t, out in ((0, down_ref), (1, up_ref)):
        out[:, 0:LANES] = jnp.where(first, keep[t], got[t]) * factor
        out[:, LANES : 2 * LANES] = jnp.where(first, got[t], keep[t]) * factor
        out[:, 2 * LANES : 3 * LANES] = total([part[t] for part in (p0, p1, p2, p3)]) * factor


def sum_call(kernel, meta, operands, shapes, after=None):
    in_specs = [SMEM] + [VMEM] * len(operands)
    operands = [meta, *operands]
    if after is not None:
        in_specs.append(ANY)
        operands.append(after)
    return pl.pallas_call(
        kernel, in_specs=in_specs, out_specs=[VMEM] * len(shapes), out_shape=shapes, compiler_params=limit(LIM)
    )(*operands)


def ring(parts, axis0, axis1):
    got = [parts[0]]
    for d in (2, 1, 3):
        got.append(shift(parts[d], axis0, axis1, d))
    return got


def local(tokens, grad_out, w_up, w_down):
    index = lax.axis_index(AXES)
    place = jnp.arange(4, dtype=jnp.int32)
    xh, z, core = index // 64, (index // 16) % 4, (index // 8) % 2
    xl, y = (index // 4) % 2, index % 4
    meta = jnp.where(place == 0, core, jnp.where(place == 1, xh * 2 + xl, jnp.where(place == 2, y, z)))
    meta = meta.astype(jnp.int32)

    preact, pack_tok = pl.pallas_call(
        preact_kernel,
        in_specs=[SMEM, ANY, ANY],
        out_specs=[VMEM] * 2,
        out_shape=[jax.ShapeDtypeStruct((TOK, HID), F32), bf16(TOK, HALF)],
        scratch_shapes=[
            pltpu.VMEM((TOK, WIDTH), BF16),
            pltpu.VMEM((WIDTH, HID), BF16),
            pltpu.SemaphoreType.DMA((2, SPANS)),
        ],
        compiler_params=limit(50),
        cost_estimate=cost(2 * TOK * HID * WIDTH, 16 * 1024 * 1024),
        name="preact",
    )(meta, tokens, w_up)
    peer_tok = swap(pack_tok)

    hid, pack_grad = pl.pallas_call(
        hidden_kernel,
        in_specs=[SMEM, ANY, ANY, VMEM],
        out_specs=[VMEM] * 2,
        out_shape=[bf16(HID, 2 * TOK), bf16(TOK, HALF)],
        scratch_shapes=[
            pltpu.VMEM((HID, TOK), F32),
            pltpu.VMEM((HID, TOK), F32),
            pltpu.VMEM((TOK, WIDTH), BF16),
            pltpu.VMEM((HID, WIDTH), BF16),
            pltpu.SemaphoreType.DMA((2, SPANS)),
        ],
        compiler_params=limit(44),
        cost_estimate=cost(2 * TOK * HID * WIDTH, 18 * 1024 * 1024),
        name="hidden",
    )(meta, grad_out, w_down, preact)
    hid_peer = swap(hid)
    peer_grad = swap(pack_grad)

    up = term_call(meta, 1, hid, hid_peer, tokens, peer_tok)
    down = term_call(meta, 0, hid, hid_peer, grad_out, peer_grad)
    up_major, up_minor = ring(up[:4], "x", "y"), ring(up[4:], "z", "z")
    major, minor = ring(down[:4], "x", "y"), ring(down[4:], "z", "z")

    major = sum_call(major1_kernel, meta, major + up_major, [bf16(2, 4, 2, SUB, LANES)] * 4)
    minor = sum_call(minor1_kernel, meta, minor + up_minor, [bf16(2, 4, SUB, LANES)] * 4, major[0])
    major, last = ring(major, "y", "z"), minor[0]
    minor = ring(minor, "x", "x")
    major = sum_call(major2_kernel, meta, major, [bf16(2, 2, SUB, LANES)] * 4, last)
    minor = sum_call(minor2_kernel, meta, minor, [bf16(2, SUB, LANES)] * 4, major[0])
    major, last = ring(major, "z", "x"), minor[0]
    minor = ring(minor, "y", "y")
    keep, send = sum_call(major3_kernel, meta, major, [jax.ShapeDtypeStruct((2, SUB, LANES), F32)] * 2, last)
    total_tokens = tokens.shape[0] * lax.axis_size("row") * lax.axis_size("col")
    up, down = sum_call(
        functools.partial(final_kernel, factor=1.0 / math.sqrt(total_tokens)),
        meta, [keep, swap(send)] + minor,
        [jax.ShapeDtypeStruct((SUB, COLORS * LANES), F32)] * 2,
    )
    return up.T, down.T


def solution(mesh):
    placed = (P(AXES, None), P(AXES, None), P(), P())
    return jax.shard_map(
        local,
        mesh=mesh,
        in_specs=placed,
        out_specs=(P("row", "col"), P("row", "col")),
        check_vma=False,
    )
```

```python
import functools
import math

import jax
import jax.numpy as jnp
from jax import lax
from jax.experimental import pallas as pl
from jax.experimental.pallas import tpu as pltpu
from jax.sharding import PartitionSpec as P


AXES = ("row", "col")
TOK = 512
HID = 512
WIDTH = 6144
LANES = 128
SUB = 64
COLORS = 3
HALF = WIDTH // 2
BF16 = jnp.bfloat16
F32 = jnp.float32


def coords(index):
    row, col = divmod(index, 8)
    xh, rest = divmod(row, 8)
    z, core = divmod(rest, 2)
    xl, y = divmod(col, 4)
    return xh * 2 + xl, y, z, core


def linear(x, y, z, core):
    x, y, z = x % 4, y % 4, z % 4
    return ((x // 2) * 8 + z * 2 + core) * 8 + (x % 2) * 4 + y


def shift(value, axis0, axis1, step):
    pairs = []
    for index in range(128):
        x, y, z, core = coords(index)
        place = {"x": x, "y": y, "z": z}
        place[axis0 if core == 0 else axis1] ^= step
        pairs.append((index, linear(place["x"], place["y"], place["z"], core)))
    return lax.ppermute(value, AXES, pairs)


def swap(value):
    pairs = []
    for index in range(128):
        x, y, z, core = coords(index)
        pairs.append((index, linear(x, y, z, 1 - core)))
    return lax.ppermute(value, AXES, pairs)


def limit(mib):
    return pltpu.CompilerParams(vmem_limit_bytes=mib * 1024 * 1024)


def cost(flops, bytes_accessed):
    return pl.CostEstimate(flops=flops, bytes_accessed=bytes_accessed, transcendentals=0)


VMEM = pl.BlockSpec(memory_space=pltpu.VMEM)
SMEM = pl.BlockSpec(memory_space=pltpu.SMEM)
ANY = pl.BlockSpec(memory_space=pl.ANY)
LIM = 12
CHUNK = 2 * COLORS * LANES
AHEAD = 5
SPANS = ((0, 768), (768, 1536), (2304, 1536), (3840, 1536), (5376, 768))


def pack_columns(meta, step, block_ref, peer_ref):
    core, own_z = meta[0], meta[3]
    xh, z = step // 4, step % 4
    j = z ^ own_z
    base = step * CHUNK
    for cp in range(2):
        source = pl.multiple_of(base + cp * 384 + (1 - core) * LANES, LANES)
        target = pl.multiple_of((j * 4 + xh * 2 + cp) * LANES, LANES)
        peer_ref[:, pl.ds(target, LANES)] = block_ref[:, pl.ds(source, LANES)]
    source = pl.multiple_of(base + (1 - core) * 384 + 2 * LANES, LANES)
    target = pl.multiple_of((16 + j * 2 + xh) * LANES, LANES)
    peer_ref[:, pl.ds(target, LANES)] = block_ref[:, pl.ds(source, LANES)]


def copies(rows_ref, w_ref, w_axis, rows_buf, w_buf, sems):
    def pair(step):
        at = pl.ds(*SPANS[step])
        w_at = (at, slice(None)) if w_axis == 0 else (slice(None), at)
        return (
            pltpu.make_async_copy(rows_ref.at[:, at], rows_buf.at[:, at], sems.at[0, step]),
            pltpu.make_async_copy(w_ref.at[*w_at], w_buf.at[*w_at], sems.at[1, step]),
        )

    return pair


def stream(pair, work):
    for step in range(AHEAD):
        for copy in pair(step):
            copy.start()
    for step, (first, width) in enumerate(SPANS):
        for copy in pair(step):
            copy.wait()
        if step + AHEAD < len(SPANS):
            for copy in pair(step + AHEAD):
                copy.start()
        work(step, pl.ds(first, width), range(first // CHUNK, (first + width) // CHUNK))


def preact_kernel(meta, tok_ref, w_ref, out_ref, peer_ref, tok_buf, w_buf, sems):
    def work(step, at, groups):
        part = jnp.dot(tok_buf[:, at], w_buf[at, :], preferred_element_type=F32)
        if step == 0:
            out_ref[...] = part
        else:
            out_ref[...] += part
        for group in groups:
            pack_columns(meta, group, tok_buf, peer_ref)

    stream(copies(tok_ref, w_ref, 0, tok_buf, w_buf, sems), work)


def hidden_kernel(
    meta, grad_ref, w_ref, preact_ref, act_ref, hid_ref, peer_ref, acc_ref, slope_ref, grad_buf, w_buf, sems
):
    def gelu(block):
        rows = pl.ds(block * LANES, LANES)
        preact = preact_ref[rows, :].T
        cumul = 0.5 * (1.0 + lax.erf(preact * (1.0 / math.sqrt(2.0))))
        density = jnp.exp(-0.5 * preact * preact) * (1.0 / math.sqrt(2.0 * math.pi))
        act_ref[:, rows] = (preact * cumul).astype(BF16)
        slope_ref[:, rows] = cumul + preact * density

    def work(step, at, groups):
        if step < TOK // LANES:
            gelu(step)
        part = lax.dot_general(
            w_buf[:, at], grad_buf[:, at], (((1,), (1,)), ((), ())), preferred_element_type=F32
        )
        if step == 0:
            acc_ref[...] = part
        elif step + 1 < len(SPANS):
            acc_ref[...] += part
        else:
            hid_ref[...] = ((acc_ref[...] + part) * slope_ref[...]).astype(BF16)
        for group in groups:
            pack_columns(meta, group, grad_buf, peer_ref)

    stream(copies(grad_ref, w_ref, 1, grad_buf, w_buf, sems), work)


def term_kernel(meta, *refs):
    hid, hid_peer, full, peer = refs[:4]
    major, minor, scr = refs[4:8], refs[8:12], refs[12]
    core, own_x, own_y, own_z = meta[0], meta[1], meta[2], meta[3]

    def rows(x, y):
        return pl.ds(pl.multiple_of((x % 2) * 256 + y * SUB, SUB), SUB)

    def matmul(step, slot):
        tiles = []
        for q in range(4):
            if step < 4:
                group = (q // 2) * 8 + (own_z ^ step) * 2 + q % 2
                column = group * 384 + core * LANES
            else:
                group = (q % 2) * 8 + (own_z ^ ((step - 4) * 2 + q // 2)) * 2 + core
                column = group * 384 + 2 * LANES
            tiles.append(full[:, pl.ds(pl.multiple_of(column, LANES), LANES)])
        own = jnp.concatenate(tiles, axis=1)
        acc = jnp.dot(hid[...], own, preferred_element_type=F32)
        other = peer[:, step * 4 * LANES : (step + 1) * 4 * LANES]
        acc += jnp.dot(hid_peer[...], other, preferred_element_type=F32)
        acc = acc.astype(BF16)
        for q in range(4):
            scr[slot, q] = acc[:, q * LANES : (q + 1) * LANES]

    def scatter(step, slot):
        if step < 4:
            for d in range(4):
                for w in range(4):
                    x = own_x ^ jnp.where(core == 0, d, w)
                    y = own_y ^ jnp.where(core == 0, w, d)
                    for cp in range(2):
                        major[d][step, cp, w] = scr[slot, (x // 2) * 2 + cp, rows(x, y), :]
            return
        for jj in range(2):
            for xo in range(4):
                x = own_x ^ xo
                for yo in range(4):
                    y = own_y ^ yo
                    minor[(step - 4) * 2 + jj][xo, yo] = scr[slot, jj * 2 + x // 2, rows(x, y), :]

    matmul(0, 0)
    for step in range(1, 6):
        matmul(step, step % 2)
        scatter(step - 1, (step - 1) % 2)
    scatter(5, 1)


MAJOR1 = (4, 2, 4, SUB, LANES)
MINOR1 = (4, 4, SUB, LANES)


def bf16(*dims):
    return jax.ShapeDtypeStruct(dims, BF16)


def term_call(meta, hid, hid_peer, full, peer):
    return pl.pallas_call(
        term_kernel,
        in_specs=[SMEM] + [VMEM] * 4,
        out_specs=[VMEM] * 8,
        out_shape=[bf16(*MAJOR1)] * 4 + [bf16(*MINOR1)] * 4,
        scratch_shapes=[pltpu.VMEM((2, 4, HID, LANES), BF16)],
        compiler_params=limit(LIM),
        cost_estimate=cost(4 * TOK * HID * HALF, 12 * 1024 * 1024),
    )(meta, hid, hid_peer, full, peer)


def total(pieces):
    out = pieces[0].astype(F32)
    for piece in pieces[1:]:
        out += piece.astype(F32)
    return out


def major1_kernel(meta, *refs):
    core = meta[0]
    terms, out = (refs[0:4], refs[4:8]), refs[8:12]
    for e in range(4):

        def body(f, _):
            j = jnp.where(core == 0, f, e)
            w = jnp.where(core == 0, e, f)
            for t in range(2):
                for cp in range(2):
                    out[e][t, f, cp] = total([part[j, cp, w] for part in terms[t]]).astype(BF16)
            return 0

        lax.fori_loop(0, 4, body, 0)


def minor1_kernel(meta, *refs):
    terms, out = (refs[0:4], refs[4:8]), refs[9:13]
    for e in range(4):

        def body(f, _):
            for t in range(2):
                out[e][t, f] = total([part[e, f] for part in terms[t]]).astype(BF16)
            return 0

        lax.fori_loop(0, 4, body, 0)


def major2_kernel(meta, *refs):
    parts, out = refs[:4], refs[5:9]
    for f in range(4):
        for t in range(2):
            for cp in range(2):
                out[f][t, cp] = total([part[t, f, cp] for part in parts]).astype(BF16)


def minor2_kernel(meta, *refs):
    parts, out = refs[:4], refs[5:9]
    for f in range(4):
        for t in range(2):
            out[f][t] = total([part[t, f] for part in parts]).astype(BF16)


def major3_kernel(meta, *refs):
    parts, (keep, send) = refs[:4], refs[5:7]
    core = meta[0]
    for t in range(2):
        keep[t] = total([part[t, core] for part in parts])
        send[t] = total([part[t, 1 - core] for part in parts])


def final_kernel(meta, keep, got, p0, p1, p2, p3, up_ref, down_ref, *, factor):
    first = meta[0] == 0
    for t, out in ((0, down_ref), (1, up_ref)):
        out[:, 0:LANES] = jnp.where(first, keep[t], got[t]) * factor
        out[:, LANES : 2 * LANES] = jnp.where(first, got[t], keep[t]) * factor
        out[:, 2 * LANES : 3 * LANES] = total([part[t] for part in (p0, p1, p2, p3)]) * factor


def sum_call(kernel, meta, operands, shapes, after=None):
    in_specs = [SMEM] + [VMEM] * len(operands)
    operands = [meta, *operands]
    if after is not None:
        in_specs.append(ANY)
        operands.append(after)
    return pl.pallas_call(
        kernel,
        in_specs=in_specs,
        out_specs=[VMEM] * len(shapes),
        out_shape=shapes,
        compiler_params=limit(LIM),
    )(*operands)


def ring(parts, axis0, axis1):
    got = [parts[0]]
    for d in (2, 1, 3):
        got.append(shift(parts[d], axis0, axis1, d))
    return got


def local(tokens, grad_out, w_up, w_down):
    index = lax.axis_index(AXES)
    place = jnp.arange(4, dtype=jnp.int32)
    xh, z, core = index // 64, (index // 16) % 4, (index // 8) % 2
    xl, y = (index // 4) % 2, index % 4
    meta = jnp.where(place == 0, core, jnp.where(place == 1, xh * 2 + xl, jnp.where(place == 2, y, z)))
    meta = meta.astype(jnp.int32)

    preact, pack_tok = pl.pallas_call(
        preact_kernel,
        in_specs=[SMEM, ANY, ANY],
        out_specs=[VMEM] * 2,
        out_shape=[jax.ShapeDtypeStruct((TOK, HID), F32), bf16(TOK, HALF)],
        scratch_shapes=[
            pltpu.VMEM((TOK, WIDTH), BF16),
            pltpu.VMEM((WIDTH, HID), BF16),
            pltpu.SemaphoreType.DMA((2, len(SPANS))),
        ],
        compiler_params=limit(50),
        cost_estimate=cost(2 * TOK * HID * WIDTH, 16 * 1024 * 1024),
        name="preact",
    )(meta, tokens, w_up)
    peer_tok = swap(pack_tok)

    act, hid, pack_grad = pl.pallas_call(
        hidden_kernel,
        in_specs=[SMEM, ANY, ANY, VMEM],
        out_specs=[VMEM] * 3,
        out_shape=[bf16(HID, TOK), bf16(HID, TOK), bf16(TOK, HALF)],
        scratch_shapes=[
            pltpu.VMEM((HID, TOK), F32),
            pltpu.VMEM((HID, TOK), F32),
            pltpu.VMEM((TOK, WIDTH), BF16),
            pltpu.VMEM((HID, WIDTH), BF16),
            pltpu.SemaphoreType.DMA((2, len(SPANS))),
        ],
        compiler_params=limit(44),
        cost_estimate=cost(2 * TOK * HID * WIDTH, 18 * 1024 * 1024),
        name="hidden",
    )(meta, grad_out, w_down, preact)
    hid_peer = swap(hid)
    act_peer = swap(act)
    peer_grad = swap(pack_grad)

    up = term_call(meta, hid, hid_peer, tokens, peer_tok)
    down = term_call(meta, act, act_peer, grad_out, peer_grad)
    up_major, up_minor = ring(up[:4], "x", "y"), ring(up[4:], "z", "z")
    major, minor = ring(down[:4], "x", "y"), ring(down[4:], "z", "z")

    major = sum_call(major1_kernel, meta, major + up_major, [bf16(2, 4, 2, SUB, LANES)] * 4)
    minor = sum_call(minor1_kernel, meta, minor + up_minor, [bf16(2, 4, SUB, LANES)] * 4, major[0])
    major, last = ring(major, "y", "z"), minor[0]
    minor = ring(minor, "x", "x")
    major = sum_call(major2_kernel, meta, major, [bf16(2, 2, SUB, LANES)] * 4, last)
    minor = sum_call(minor2_kernel, meta, minor, [bf16(2, SUB, LANES)] * 4, major[0])
    major, last = ring(major, "z", "x"), minor[0]
    minor = ring(minor, "y", "y")
    keep, send = sum_call(
        major3_kernel, meta, major, [jax.ShapeDtypeStruct((2, SUB, LANES), F32)] * 2, last
    )
    total_tokens = tokens.shape[0] * lax.axis_size("row") * lax.axis_size("col")
    up, down = sum_call(
        functools.partial(final_kernel, factor=1.0 / math.sqrt(total_tokens)),
        meta, [keep, swap(send)] + minor,
        [jax.ShapeDtypeStruct((SUB, COLORS * LANES), F32)] * 2,
    )
    return up.T, down.T


def solution(mesh):
    placed = (P(AXES, None), P(AXES, None), P(), P())
    return jax.shard_map(
        local,
        mesh=mesh,
        in_specs=placed,
        out_specs=(P("row", "col"), P("row", "col")),
        check_vma=False,
    )
```

```python
import functools
import math

import jax
import jax.numpy as jnp
from jax import lax
from jax.experimental import pallas as pl
from jax.experimental.pallas import tpu as pltpu
from jax.sharding import PartitionSpec as P


AXES = ("row", "col")
TOK = 512
HID = 512
WIDTH = 6144
LANES = 128
SUB = 64
COLORS = 3
HALF = WIDTH // 2
BF16 = jnp.bfloat16
F32 = jnp.float32


def coords(index):
    row, col = divmod(index, 8)
    xh, rest = divmod(row, 8)
    z, core = divmod(rest, 2)
    xl, y = divmod(col, 4)
    return xh * 2 + xl, y, z, core


def linear(x, y, z, core):
    x, y, z = x % 4, y % 4, z % 4
    return ((x // 2) * 8 + z * 2 + core) * 8 + (x % 2) * 4 + y


def shift(value, axis0, axis1, step):
    pairs = []
    for index in range(128):
        x, y, z, core = coords(index)
        place = {"x": x, "y": y, "z": z}
        place[axis0 if core == 0 else axis1] ^= step
        pairs.append((index, linear(place["x"], place["y"], place["z"], core)))
    return lax.ppermute(value, AXES, pairs)


def swap(value):
    pairs = []
    for index in range(128):
        x, y, z, core = coords(index)
        pairs.append((index, linear(x, y, z, 1 - core)))
    return lax.ppermute(value, AXES, pairs)


def here():
    row, col = lax.axis_index("row"), lax.axis_index("col")
    return row % 2, row // 8 * 2 + col // 4, col % 4, row // 2 % 4


def limit(mib):
    return pltpu.CompilerParams(vmem_limit_bytes=mib * 1024 * 1024)


def cost(flops, bytes_accessed):
    return pl.CostEstimate(flops=flops, bytes_accessed=bytes_accessed, transcendentals=0)


VMEM = pl.BlockSpec(memory_space=pltpu.VMEM)
ANY = pl.BlockSpec(memory_space=pl.ANY)
LIM = 12
CHUNK = 2 * COLORS * LANES
AHEAD = 5
SPANS = ((0, 768), (768, 1536), (2304, 1536), (3840, 1536), (5376, 768))


def pack_columns(step, block_ref, peer_ref):
    core, _, _, own_z = here()
    xh, z = step // 4, step % 4
    j = z ^ own_z
    base = step * CHUNK
    for cp in range(2):
        source = pl.multiple_of(base + cp * 384 + (1 - core) * LANES, LANES)
        target = pl.multiple_of((j * 4 + xh * 2 + cp) * LANES, LANES)
        peer_ref[:, pl.ds(target, LANES)] = block_ref[:, pl.ds(source, LANES)]
    source = pl.multiple_of(base + (1 - core) * 384 + 2 * LANES, LANES)
    target = pl.multiple_of((16 + j * 2 + xh) * LANES, LANES)
    peer_ref[:, pl.ds(target, LANES)] = block_ref[:, pl.ds(source, LANES)]


def copies(rows_ref, w_ref, w_axis, rows_buf, w_buf, sems):
    def pair(step):
        at = pl.ds(*SPANS[step])
        w_at = (at, slice(None)) if w_axis == 0 else (slice(None), at)
        return (
            pltpu.make_async_copy(rows_ref.at[:, at], rows_buf.at[:, at], sems.at[0, step]),
            pltpu.make_async_copy(w_ref.at[*w_at], w_buf.at[*w_at], sems.at[1, step]),
        )

    return pair


def stream(pair, work):
    for step in range(AHEAD):
        for copy in pair(step):
            copy.start()
    for step, (first, width) in enumerate(SPANS):
        for copy in pair(step):
            copy.wait()
        if step + AHEAD < len(SPANS):
            for copy in pair(step + AHEAD):
                copy.start()
        work(step, pl.ds(first, width), range(first // CHUNK, (first + width) // CHUNK))


def preact_kernel(tok_ref, w_ref, out_ref, peer_ref, tok_buf, w_buf, sems):
    def work(step, at, groups):
        part = jnp.dot(tok_buf[:, at], w_buf[at, :], preferred_element_type=F32)
        if step == 0:
            out_ref[...] = part
        else:
            out_ref[...] += part
        for group in groups:
            pack_columns(group, tok_buf, peer_ref)

    stream(copies(tok_ref, w_ref, 0, tok_buf, w_buf, sems), work)


def hidden_kernel(
    grad_ref, w_ref, preact_ref, act_ref, hid_ref, peer_ref, acc_ref, slope_ref, grad_buf, w_buf, sems
):
    def gelu(block):
        rows = pl.ds(block * LANES, LANES)
        preact = preact_ref[rows, :].T
        cumul = 0.5 * (1.0 + lax.erf(preact * (1.0 / math.sqrt(2.0))))
        density = jnp.exp(-0.5 * preact * preact) * (1.0 / math.sqrt(2.0 * math.pi))
        act_ref[:, rows] = (preact * cumul).astype(BF16)
        slope_ref[:, rows] = cumul + preact * density

    def work(step, at, groups):
        if step < TOK // LANES:
            gelu(step)
        part = lax.dot_general(
            w_buf[:, at], grad_buf[:, at], (((1,), (1,)), ((), ())), preferred_element_type=F32
        )
        if step == 0:
            acc_ref[...] = part
        elif step + 1 < len(SPANS):
            acc_ref[...] += part
        else:
            hid_ref[...] = ((acc_ref[...] + part) * slope_ref[...]).astype(BF16)
        for group in groups:
            pack_columns(group, grad_buf, peer_ref)

    stream(copies(grad_ref, w_ref, 1, grad_buf, w_buf, sems), work)


def term_kernel(*refs):
    hid, hid_peer, full, peer = refs[:4]
    major, minor, scr = refs[4:8], refs[8:12], refs[12]
    core, own_x, own_y, own_z = here()

    def rows(x, y):
        return pl.ds(pl.multiple_of((x % 2) * 256 + y * SUB, SUB), SUB)

    def matmul(step, slot):
        tiles = []
        for q in range(4):
            if step < 4:
                group = (q // 2) * 8 + (own_z ^ step) * 2 + q % 2
                column = group * 384 + core * LANES
            else:
                group = (q % 2) * 8 + (own_z ^ ((step - 4) * 2 + q // 2)) * 2 + core
                column = group * 384 + 2 * LANES
            tiles.append(full[:, pl.ds(pl.multiple_of(column, LANES), LANES)])
        own = jnp.concatenate(tiles, axis=1)
        acc = jnp.dot(hid[...], own, preferred_element_type=F32)
        other = peer[:, step * 4 * LANES : (step + 1) * 4 * LANES]
        acc += jnp.dot(hid_peer[...], other, preferred_element_type=F32)
        acc = acc.astype(BF16)
        for q in range(4):
            scr[slot, q] = acc[:, q * LANES : (q + 1) * LANES]

    def scatter(step, slot):
        if step < 4:
            for d in range(4):
                for w in range(4):
                    x = own_x ^ jnp.where(core == 0, d, w)
                    y = own_y ^ jnp.where(core == 0, w, d)
                    for cp in range(2):
                        major[d][step, cp, w] = scr[slot, (x // 2) * 2 + cp, rows(x, y), :]
            return
        for jj in range(2):
            for xo in range(4):
                x = own_x ^ xo
                for yo in range(4):
                    y = own_y ^ yo
                    minor[(step - 4) * 2 + jj][xo, yo] = scr[slot, jj * 2 + x // 2, rows(x, y), :]

    matmul(0, 0)
    for step in range(1, 6):
        matmul(step, step % 2)
        scatter(step - 1, (step - 1) % 2)
    scatter(5, 1)


MAJOR1 = (4, 2, 4, SUB, LANES)
MINOR1 = (4, 4, SUB, LANES)


def bf16(*dims):
    return jax.ShapeDtypeStruct(dims, BF16)


def term_call(hid, hid_peer, full, peer):
    return pl.pallas_call(
        term_kernel,
        in_specs=[VMEM] * 4,
        out_specs=[VMEM] * 8,
        out_shape=[bf16(*MAJOR1)] * 4 + [bf16(*MINOR1)] * 4,
        scratch_shapes=[pltpu.VMEM((2, 4, HID, LANES), BF16)],
        compiler_params=limit(LIM),
        cost_estimate=cost(4 * TOK * HID * HALF, 12 * 1024 * 1024),
    )(hid, hid_peer, full, peer)


def total(pieces):
    out = pieces[0].astype(F32)
    for piece in pieces[1:]:
        out += piece.astype(F32)
    return out


def major1_kernel(*refs):
    core = here()[0]
    terms, out = (refs[0:4], refs[4:8]), refs[8:12]
    for e in range(4):

        def body(f, _):
            j = jnp.where(core == 0, f, e)
            w = jnp.where(core == 0, e, f)
            for t in range(2):
                for cp in range(2):
                    out[e][t, f, cp] = total([part[j, cp, w] for part in terms[t]]).astype(BF16)
            return 0

        lax.fori_loop(0, 4, body, 0)


def minor1_kernel(*refs):
    terms, out = (refs[0:4], refs[4:8]), refs[9:13]
    for e in range(4):

        def body(f, _):
            for t in range(2):
                out[e][t, f] = total([part[e, f] for part in terms[t]]).astype(BF16)
            return 0

        lax.fori_loop(0, 4, body, 0)


def major2_kernel(*refs):
    parts, out = refs[:4], refs[5:9]
    for f in range(4):
        for t in range(2):
            for cp in range(2):
                out[f][t, cp] = total([part[t, f, cp] for part in parts]).astype(BF16)


def minor2_kernel(*refs):
    parts, out = refs[:4], refs[5:9]
    for f in range(4):
        for t in range(2):
            out[f][t] = total([part[t, f] for part in parts]).astype(BF16)


def major3_kernel(*refs):
    parts, (keep, send) = refs[:4], refs[5:7]
    core = here()[0]
    for t in range(2):
        keep[t] = total([part[t, core] for part in parts])
        send[t] = total([part[t, 1 - core] for part in parts])


def final_kernel(keep, got, p0, p1, p2, p3, up_ref, down_ref, *, factor):
    first = here()[0] == 0
    for t, out in ((0, down_ref), (1, up_ref)):
        out[:, 0:LANES] = jnp.where(first, keep[t], got[t]) * factor
        out[:, LANES : 2 * LANES] = jnp.where(first, got[t], keep[t]) * factor
        out[:, 2 * LANES : 3 * LANES] = total([part[t] for part in (p0, p1, p2, p3)]) * factor


def sum_call(kernel, operands, shapes, after=None):
    in_specs = [VMEM] * len(operands)
    operands = list(operands)
    if after is not None:
        in_specs.append(ANY)
        operands.append(after)
    return pl.pallas_call(
        kernel,
        in_specs=in_specs,
        out_specs=[VMEM] * len(shapes),
        out_shape=shapes,
        compiler_params=limit(LIM),
    )(*operands)


def ring(parts, axis0, axis1):
    got = [parts[0]]
    for d in (2, 1, 3):
        got.append(shift(parts[d], axis0, axis1, d))
    return got


def local(tokens, grad_out, w_up, w_down):
    preact, pack_tok = pl.pallas_call(
        preact_kernel,
        in_specs=[ANY, ANY],
        out_specs=[VMEM] * 2,
        out_shape=[jax.ShapeDtypeStruct((TOK, HID), F32), bf16(TOK, HALF)],
        scratch_shapes=[
            pltpu.VMEM((TOK, WIDTH), BF16),
            pltpu.VMEM((WIDTH, HID), BF16),
            pltpu.SemaphoreType.DMA((2, len(SPANS))),
        ],
        compiler_params=limit(50),
        cost_estimate=cost(2 * TOK * HID * WIDTH, 16 * 1024 * 1024),
        name="preact",
    )(tokens, w_up)
    peer_tok = swap(pack_tok)

    act, hid, pack_grad = pl.pallas_call(
        hidden_kernel,
        in_specs=[ANY, ANY, VMEM],
        out_specs=[VMEM] * 3,
        out_shape=[bf16(HID, TOK), bf16(HID, TOK), bf16(TOK, HALF)],
        scratch_shapes=[
            pltpu.VMEM((HID, TOK), F32),
            pltpu.VMEM((HID, TOK), F32),
            pltpu.VMEM((TOK, WIDTH), BF16),
            pltpu.VMEM((HID, WIDTH), BF16),
            pltpu.SemaphoreType.DMA((2, len(SPANS))),
        ],
        compiler_params=limit(44),
        cost_estimate=cost(2 * TOK * HID * WIDTH, 18 * 1024 * 1024),
        name="hidden",
    )(grad_out, w_down, preact)
    hid_peer = swap(hid)
    act_peer = swap(act)
    peer_grad = swap(pack_grad)

    up = term_call(hid, hid_peer, tokens, peer_tok)
    down = term_call(act, act_peer, grad_out, peer_grad)
    up_major, up_minor = ring(up[:4], "x", "y"), ring(up[4:], "z", "z")
    major, minor = ring(down[:4], "x", "y"), ring(down[4:], "z", "z")

    major = sum_call(major1_kernel, major + up_major, [bf16(2, 4, 2, SUB, LANES)] * 4)
    minor = sum_call(minor1_kernel, minor + up_minor, [bf16(2, 4, SUB, LANES)] * 4, major[0])
    major, last = ring(major, "y", "z"), minor[0]
    minor = ring(minor, "x", "x")
    major = sum_call(major2_kernel, major, [bf16(2, 2, SUB, LANES)] * 4, last)
    minor = sum_call(minor2_kernel, minor, [bf16(2, SUB, LANES)] * 4, major[0])
    major, last = ring(major, "z", "x"), minor[0]
    minor = ring(minor, "y", "y")
    keep, send = sum_call(
        major3_kernel, major, [jax.ShapeDtypeStruct((2, SUB, LANES), F32)] * 2, last
    )
    total_tokens = tokens.shape[0] * lax.axis_size("row") * lax.axis_size("col")
    up, down = sum_call(
        functools.partial(final_kernel, factor=1.0 / math.sqrt(total_tokens)),
        [keep, swap(send)] + minor,
        [jax.ShapeDtypeStruct((SUB, COLORS * LANES), F32)] * 2,
    )
    return up.T, down.T


def solution(mesh):
    placed = (P(AXES, None), P(AXES, None), P(), P())
    return jax.shard_map(
        local,
        mesh=mesh,
        in_specs=placed,
        out_specs=(P("row", "col"), P("row", "col")),
        check_vma=False,
    )
```

```python
import functools
import math

import jax
import jax.numpy as jnp
from jax import lax
from jax.experimental import pallas as pl
from jax.experimental.pallas import tpu as pltpu
from jax.sharding import PartitionSpec as P


AXES = ("row", "col")
TOK = 512
HID = 512
WIDTH = 6144
LANES = 128
SUB = 64
COLORS = 3
HALF = WIDTH // 2
BF16 = jnp.bfloat16
F32 = jnp.float32


def coords(index):
    row, col = divmod(index, 8)
    xh, rest = divmod(row, 8)
    z, core = divmod(rest, 2)
    xl, y = divmod(col, 4)
    return xh * 2 + xl, y, z, core


def linear(x, y, z, core):
    x, y, z = x % 4, y % 4, z % 4
    return ((x // 2) * 8 + z * 2 + core) * 8 + (x % 2) * 4 + y


def shift(value, axis0, axis1, step):
    pairs = []
    for index in range(128):
        x, y, z, core = coords(index)
        place = {"x": x, "y": y, "z": z}
        place[axis0 if core == 0 else axis1] ^= step
        pairs.append((index, linear(place["x"], place["y"], place["z"], core)))
    return lax.ppermute(value, AXES, pairs)


def swap(value):
    pairs = []
    for index in range(128):
        x, y, z, core = coords(index)
        pairs.append((index, linear(x, y, z, 1 - core)))
    return lax.ppermute(value, AXES, pairs)


def here():
    row, col = lax.axis_index("row"), lax.axis_index("col")
    return row % 2, row // 8 * 2 + col // 4, col % 4, row // 2 % 4


def limit(mib):
    return pltpu.CompilerParams(vmem_limit_bytes=mib * 1024 * 1024)


def cost(flops, bytes_accessed):
    return pl.CostEstimate(flops=flops, bytes_accessed=bytes_accessed, transcendentals=0)


VMEM = pl.BlockSpec(memory_space=pltpu.VMEM)
ANY = pl.BlockSpec(memory_space=pl.ANY)
LIM = 12
CHUNK = 2 * COLORS * LANES
AHEAD = 5
SPANS = ((0, 768), (768, 1536), (2304, 1536), (3840, 1536), (5376, 768))


def pack_columns(step, block_ref, peer_ref):
    core, _, _, own_z = here()
    xh, z = step // 4, step % 4
    j = z ^ own_z
    base = step * CHUNK
    for cp in range(2):
        source = pl.multiple_of(base + cp * 384 + (1 - core) * LANES, LANES)
        target = pl.multiple_of((j * 4 + xh * 2 + cp) * LANES, LANES)
        peer_ref[:, pl.ds(target, LANES)] = block_ref[:, pl.ds(source, LANES)]
    source = pl.multiple_of(base + (1 - core) * 384 + 2 * LANES, LANES)
    target = pl.multiple_of((16 + j * 2 + xh) * LANES, LANES)
    peer_ref[:, pl.ds(target, LANES)] = block_ref[:, pl.ds(source, LANES)]


def copies(rows_ref, w_ref, w_axis, rows_buf, w_buf, sems):
    def pair(step):
        at = pl.ds(*SPANS[step])
        w_at = (at, slice(None)) if w_axis == 0 else (slice(None), at)
        return (
            pltpu.make_async_copy(rows_ref.at[:, at], rows_buf.at[:, at], sems.at[0, step]),
            pltpu.make_async_copy(w_ref.at[*w_at], w_buf.at[*w_at], sems.at[1, step]),
        )

    return pair


def stream(pair, work):
    for step in range(AHEAD):
        for copy in pair(step):
            copy.start()
    for step, (first, width) in enumerate(SPANS):
        for copy in pair(step):
            copy.wait()
        if step + AHEAD < len(SPANS):
            for copy in pair(step + AHEAD):
                copy.start()
        work(step, pl.ds(first, width), range(first // CHUNK, (first + width) // CHUNK))


def preact_kernel(tok_ref, w_ref, out_ref, peer_ref, tok_buf, w_buf, sems):
    def work(step, at, groups):
        part = jnp.dot(tok_buf[:, at], w_buf[at, :], preferred_element_type=F32)
        if step == 0:
            out_ref[...] = part
        else:
            out_ref[...] += part
        for group in groups:
            pack_columns(group, tok_buf, peer_ref)

    stream(copies(tok_ref, w_ref, 0, tok_buf, w_buf, sems), work)


def hidden_kernel(
    grad_ref, w_ref, preact_ref, act_ref, hid_ref, peer_ref, acc_ref, slope_ref, grad_buf, w_buf, sems
):
    def gelu(block):
        rows = pl.ds(block * LANES, LANES)
        preact = preact_ref[rows, :].T
        cumul = 0.5 * (1.0 + lax.erf(preact * (1.0 / math.sqrt(2.0))))
        density = jnp.exp(-0.5 * preact * preact) * (1.0 / math.sqrt(2.0 * math.pi))
        act_ref[:, rows] = (preact * cumul).astype(BF16)
        slope_ref[:, rows] = cumul + preact * density

    def work(step, at, groups):
        if step < TOK // LANES:
            gelu(step)
        part = lax.dot_general(
            w_buf[:, at], grad_buf[:, at], (((1,), (1,)), ((), ())), preferred_element_type=F32
        )
        if step == 0:
            acc_ref[...] = part
        elif step + 1 < len(SPANS):
            acc_ref[...] += part
        else:
            hid_ref[...] = ((acc_ref[...] + part) * slope_ref[...]).astype(BF16)
        for group in groups:
            pack_columns(group, grad_buf, peer_ref)

    stream(copies(grad_ref, w_ref, 1, grad_buf, w_buf, sems), work)


def own_tiles(full, step):
    core, _, _, own_z = here()
    tiles = []
    for q in range(4):
        if step < 4:
            group = (q // 2) * 8 + (own_z ^ step) * 2 + q % 2
            column = group * 384 + core * LANES
        else:
            group = (q % 2) * 8 + (own_z ^ ((step - 4) * 2 + q // 2)) * 2 + core
            column = group * 384 + 2 * LANES
        tiles.append(full[:, pl.ds(pl.multiple_of(column, LANES), LANES)])
    return jnp.concatenate(tiles, axis=1)


def own_kernel(hid, full, out):
    for step in range(4):
        out[step] = jnp.dot(hid[...], own_tiles(full, step), preferred_element_type=F32)


def term_kernel(*refs, steps, given):
    hid_peer, peer, hid, full = refs[:2] + ((None, None) if given else refs[2:4])
    base = refs[2] if given else None
    out, scr = refs[-5:-1], refs[-1]
    core, own_x, own_y, _ = here()

    def rows(x, y):
        return pl.ds(pl.multiple_of((x % 2) * 256 + y * SUB, SUB), SUB)

    def matmul(step, slot):
        if given:
            acc = base[step]
        else:
            acc = jnp.dot(hid[...], own_tiles(full, step), preferred_element_type=F32)
        other = peer[:, step * 4 * LANES : (step + 1) * 4 * LANES]
        acc += jnp.dot(hid_peer[...], other, preferred_element_type=F32)
        acc = acc.astype(BF16)
        for q in range(4):
            scr[slot, q] = acc[:, q * LANES : (q + 1) * LANES]

    def scatter(step, slot):
        if step < 4:
            for d in range(4):
                for w in range(4):
                    x = own_x ^ jnp.where(core == 0, d, w)
                    y = own_y ^ jnp.where(core == 0, w, d)
                    for cp in range(2):
                        out[d][step, cp, w] = scr[slot, (x // 2) * 2 + cp, rows(x, y), :]
            return
        for jj in range(2):
            for xo in range(4):
                x = own_x ^ xo
                for yo in range(4):
                    y = own_y ^ yo
                    out[(step - 4) * 2 + jj][xo, yo] = scr[slot, jj * 2 + x // 2, rows(x, y), :]

    matmul(steps[0], 0)
    for i, step in enumerate(steps[1:], 1):
        matmul(step, i % 2)
        scatter(steps[i - 1], (i - 1) % 2)
    scatter(steps[-1], (len(steps) - 1) % 2)


MAJOR1 = (4, 2, 4, SUB, LANES)
MINOR1 = (4, 4, SUB, LANES)


def bf16(*dims):
    return jax.ShapeDtypeStruct(dims, BF16)


def own_call(hid, full):
    return pl.pallas_call(
        own_kernel,
        in_specs=[VMEM] * 2,
        out_specs=VMEM,
        out_shape=jax.ShapeDtypeStruct((4, HID, 4 * LANES), F32),
        compiler_params=limit(LIM),
        cost_estimate=cost(2 * TOK * HID * HALF * 2 // 3, 8 * 1024 * 1024),
        name="own_term",
    )(hid, full)


def term_call(steps, hid_peer, peer, *rest):
    major = steps[0] < 4
    return pl.pallas_call(
        functools.partial(term_kernel, steps=steps, given=len(rest) == 1),
        in_specs=[VMEM] * (2 + len(rest)),
        out_specs=[VMEM] * 4,
        out_shape=[bf16(*(MAJOR1 if major else MINOR1))] * 4,
        scratch_shapes=[pltpu.VMEM((2, 4, HID, LANES), BF16)],
        compiler_params=limit(LIM),
        cost_estimate=cost(4 * TOK * HID * HALF * len(steps) // 6, 8 * 1024 * 1024),
    )(hid_peer, peer, *rest)


def total(pieces):
    out = pieces[0].astype(F32)
    for piece in pieces[1:]:
        out += piece.astype(F32)
    return out


def major1_kernel(*refs):
    core = here()[0]
    terms, out = (refs[0:4], refs[4:8]), refs[8:12]
    for e in range(4):

        def body(f, _):
            j = jnp.where(core == 0, f, e)
            w = jnp.where(core == 0, e, f)
            for t in range(2):
                for cp in range(2):
                    out[e][t, f, cp] = total([part[j, cp, w] for part in terms[t]]).astype(BF16)
            return 0

        lax.fori_loop(0, 4, body, 0)


def minor1_kernel(*refs):
    terms, out = (refs[0:4], refs[4:8]), refs[9:13]
    for e in range(4):

        def body(f, _):
            for t in range(2):
                out[e][t, f] = total([part[e, f] for part in terms[t]]).astype(BF16)
            return 0

        lax.fori_loop(0, 4, body, 0)


def major2_kernel(*refs):
    parts, out = refs[:4], refs[5:9]
    for f in range(4):
        for t in range(2):
            for cp in range(2):
                out[f][t, cp] = total([part[t, f, cp] for part in parts]).astype(BF16)


def minor2_kernel(*refs):
    parts, out = refs[:4], refs[5:9]
    for f in range(4):
        for t in range(2):
            out[f][t] = total([part[t, f] for part in parts]).astype(BF16)


def major3_kernel(*refs):
    parts, (keep, send) = refs[:4], refs[5:7]
    core = here()[0]
    for t in range(2):
        keep[t] = total([part[t, core] for part in parts])
        send[t] = total([part[t, 1 - core] for part in parts])


def final_kernel(keep, got, p0, p1, p2, p3, up_ref, down_ref, *, factor):
    first = here()[0] == 0
    for t, out in ((0, down_ref), (1, up_ref)):
        out[:, 0:LANES] = jnp.where(first, keep[t], got[t]) * factor
        out[:, LANES : 2 * LANES] = jnp.where(first, got[t], keep[t]) * factor
        out[:, 2 * LANES : 3 * LANES] = total([part[t] for part in (p0, p1, p2, p3)]) * factor


def sum_call(kernel, operands, shapes, after=None):
    in_specs = [VMEM] * len(operands)
    operands = list(operands)
    if after is not None:
        in_specs.append(ANY)
        operands.append(after)
    return pl.pallas_call(
        kernel,
        in_specs=in_specs,
        out_specs=[VMEM] * len(shapes),
        out_shape=shapes,
        compiler_params=limit(LIM),
    )(*operands)


def ring(parts, axis0, axis1):
    got = [parts[0]]
    for d in (1, 2, 3):
        got.append(shift(parts[d], axis0, axis1, d))
    return got


def local(tokens, grad_out, w_up, w_down):
    preact, pack_tok = pl.pallas_call(
        preact_kernel,
        in_specs=[ANY, ANY],
        out_specs=[VMEM] * 2,
        out_shape=[jax.ShapeDtypeStruct((TOK, HID), F32), bf16(TOK, HALF)],
        scratch_shapes=[
            pltpu.VMEM((TOK, WIDTH), BF16),
            pltpu.VMEM((WIDTH, HID), BF16),
            pltpu.SemaphoreType.DMA((2, len(SPANS))),
        ],
        compiler_params=limit(50),
        cost_estimate=cost(2 * TOK * HID * WIDTH, 16 * 1024 * 1024),
        name="preact",
    )(tokens, w_up)
    peer_tok = swap(pack_tok)

    act, hid, pack_grad = pl.pallas_call(
        hidden_kernel,
        in_specs=[ANY, ANY, VMEM],
        out_specs=[VMEM] * 3,
        out_shape=[bf16(HID, TOK), bf16(HID, TOK), bf16(TOK, HALF)],
        scratch_shapes=[
            pltpu.VMEM((HID, TOK), F32),
            pltpu.VMEM((HID, TOK), F32),
            pltpu.VMEM((TOK, WIDTH), BF16),
            pltpu.VMEM((HID, WIDTH), BF16),
            pltpu.SemaphoreType.DMA((2, len(SPANS))),
        ],
        compiler_params=limit(44),
        cost_estimate=cost(2 * TOK * HID * WIDTH, 18 * 1024 * 1024),
        name="hidden",
    )(grad_out, w_down, preact)
    hid_peer = swap(hid)
    act_peer = swap(act)
    peer_grad = swap(pack_grad)

    majors, minors = (0, 1, 2, 3), (4, 5)
    own = own_call(hid, tokens)
    up_major = term_call(majors, hid_peer, peer_tok, own)
    up_minor = term_call(minors, hid_peer, peer_tok, hid, tokens)
    major = term_call(majors, act_peer, peer_grad, act, grad_out)
    minor = term_call(minors, act_peer, peer_grad, act, grad_out)
    up_major, up_minor = ring(up_major, "x", "y"), ring(up_minor, "z", "z")
    major, minor = ring(major, "x", "y"), ring(minor, "z", "z")

    major = sum_call(major1_kernel, major + up_major, [bf16(2, 4, 2, SUB, LANES)] * 4)
    minor = sum_call(minor1_kernel, minor + up_minor, [bf16(2, 4, SUB, LANES)] * 4, major[0])
    major, last = ring(major, "y", "z"), minor[0]
    minor = ring(minor, "x", "x")
    major = sum_call(major2_kernel, major, [bf16(2, 2, SUB, LANES)] * 4, last)
    minor = sum_call(minor2_kernel, minor, [bf16(2, SUB, LANES)] * 4, major[0])
    major, last = ring(major, "z", "x"), minor[0]
    minor = ring(minor, "y", "y")
    keep, send = sum_call(
        major3_kernel, major, [jax.ShapeDtypeStruct((2, SUB, LANES), F32)] * 2, last
    )
    total_tokens = tokens.shape[0] * lax.axis_size("row") * lax.axis_size("col")
    up, down = sum_call(
        functools.partial(final_kernel, factor=1.0 / math.sqrt(total_tokens)),
        [keep, swap(send)] + minor,
        [jax.ShapeDtypeStruct((SUB, COLORS * LANES), F32)] * 2,
    )
    return up.T, down.T


def solution(mesh):
    placed = (P(AXES, None), P(AXES, None), P(), P())
    return jax.shard_map(
        local,
        mesh=mesh,
        in_specs=placed,
        out_specs=(P("row", "col"), P("row", "col")),
        check_vma=False,
    )
```
